32 devices in a mesh: rep: 4 (over x, y), dp: 8 (over z, core).
Axes of the slice: x: 2, y: 2, z: 4, core: 2. Of those that a mesh axis runs over, the one named last changes fastest.
Arguments:
- x: bfloat16 [32, 2048, 640], P(('rep', 'dp')), parts along dimension 0
- dy: bfloat16 [32, 2048, 640], P(('rep', 'dp')), parts along dimension 0
- w_gate: bfloat16 [2, 640, 2048], replicated
- w_up: bfloat16 [2, 640, 2048], replicated
- w_down: bfloat16 [2, 2048, 640], replicated
- m_w_gate: float32 [2, 640, 2048], replicated
- m_w_up: float32 [2, 640, 2048], replicated
- m_w_down: float32 [2, 2048, 640], replicated
- v_w_gate: float32 [2, 640, 2048], replicated
- v_w_up: float32 [2, 640, 2048], replicated
- v_w_down: float32 [2, 2048, 640], replicated
Outputs:
- output 1: bfloat16 [8, 640, 2048], P('rep'), parts along dimension 0
- output 2: bfloat16 [8, 640, 2048], P('rep'), parts along dimension 0
- output 3: bfloat16 [8, 2048, 640], P('rep'), parts along dimension 0
- output 4: float32 [8, 640, 2048], P('rep'), parts along dimension 0
- output 5: float32 [8, 640, 2048], P('rep'), parts along dimension 0
- output 6: float32 [8, 2048, 640], P('rep'), parts along dimension 0
- output 7: float32 [8, 640, 2048], P('rep'), parts along dimension 0
- output 8: float32 [8, 640, 2048], P('rep'), parts along dimension 0
- output 9: float32 [8, 2048, 640], P('rep'), parts along dimension 0
There are 4 independent parts. The reference program is written for one: setup_inputs(seed, part) draws one part's arguments, and reference() takes and returns one part's arrays. A program takes and returns all parts, laid end to end along the dimension named above; an argument that names none is the same for every part.
All inputs are finite; a program needn't handle non-finite values.
Results may differ from the reference program's by a relative error of at most 0.022.
Values are sent between devices in bfloat16 or wider.
A program may use at most 2.25 GiB of HBM per device.

```python
import jax
import jax.numpy as jnp
from jax import lax

SEQUENCES = 8
TOKENS = 2048
D = 640
FF = 2048
LAYERS = 2
NAMES = ("w_gate", "w_up", "w_down")
SHAPES = {"w_gate": (LAYERS, D, FF), "w_up": (LAYERS, D, FF), "w_down": (LAYERS, FF, D)}


def bump(key, n, height):
    away = (jnp.arange(n, dtype=jnp.int32) - jax.random.randint(key, (), 0, n, jnp.int32)) % n
    return jnp.where(away < n // 8, height, 1.0)


def together(key, own, strength):
    shared = jax.random.normal(key, own.shape[1:], jnp.float32)
    return (own + strength * shared) * lax.rsqrt(1 + strength * strength)


def setup_inputs(seed: int = 0, part: int = 0) -> dict:
    kx, kdy, ka, kb, kz, kf, kh, kl, *keys = jax.random.split(jax.random.key(seed), 8 + 3 * len(NAMES))
    kx, kdy, ka, kb = (jax.random.fold_in(k, part) for k in (kx, kdy, ka, kb))
    kw, km, kv = (keys[i::3] for i in range(3))
    shape = (SEQUENCES, TOKENS, D)
    much_x, much_dy = jax.random.uniform(kz, (2,), jnp.float32, 0.0, 1.0)
    loud = 2.0 ** jax.random.uniform(jax.random.fold_in(kz, 1), (), jnp.float32, -1.0, 2.0)
    layers = 2.0 ** jax.random.uniform(kl, (LAYERS, 1, 1), jnp.float32, -1.0, 1.0)
    x = together(ka, jax.random.normal(kx, shape, jnp.float32), much_x) * bump(kf, D, 4.0)
    dy = together(kb, jax.random.normal(kdy, shape, jnp.float32), much_dy)
    drawn = {"x": x.astype(jnp.bfloat16), "dy": (loud * dy * (SEQUENCES * TOKENS) ** -0.5).astype(jnp.bfloat16)}
    for key, name in zip(kw, NAMES, strict=True):
        w = jax.random.normal(key, SHAPES[name], jnp.float32) * SHAPES[name][1] ** -0.5
        drawn[name] = (w * {"w_gate": 1.0, "w_up": bump(kh, FF, 4.0), "w_down": layers}[name]).astype(jnp.bfloat16)
    for key, name in zip(km, NAMES, strict=True):
        drawn[f"m_{name}"] = 0.1 * jax.random.normal(key, SHAPES[name], jnp.float32)
    for key, name in zip(kv, NAMES, strict=True):
        drawn[f"v_{name}"] = jax.random.uniform(key, SHAPES[name], jnp.float32, 0.005, 0.015)
    return drawn


def matmul(a, w):
    return jnp.dot(a, w, preferred_element_type=jnp.float32).astype(jnp.bfloat16)


def normed(h):
    wide = h.astype(jnp.float32)
    scale = lax.rsqrt(jnp.mean(wide**2, -1, keepdims=True) + 1e-6)
    return (wide * scale).astype(jnp.bfloat16)


def layer(h, w):
    a = normed(h)
    gate = jnp.dot(a, w["w_gate"], preferred_element_type=jnp.float32)
    up = jnp.dot(a, w["w_up"], preferred_element_type=jnp.float32)
    return h + matmul((jax.nn.silu(gate) * up).astype(jnp.bfloat16), w["w_down"])


def adamw(w, m, v, g):
    m = 0.9 * m + 0.1 * g
    v = 0.95 * v + 0.05 * g * g
    step = m * lax.rsqrt(v + 1e-8) + 0.1 * w
    return (w - 0.02 * step).astype(jnp.bfloat16), m, v


def clipped(gradients, sum_of_squares, count):
    factor = jnp.minimum(1.0, 0.5 * lax.rsqrt(sum_of_squares / count + 1e-30))
    return [g * factor for g in gradients]


def stack(weights, h):
    return lax.scan(lambda h, w: (layer(h, w), None), h, weights)[0]


def reference(x, dy, w_gate, w_up, w_down, m_w_gate, m_w_up, m_w_down, v_w_gate, v_w_up, v_w_down):
    weights = dict(zip(NAMES, (w_gate, w_up, w_down), strict=True))

    def take(so_far, sequence):
        h, by_y = sequence
        _, back = jax.vjp(lambda w: stack(w, h), weights)
        return jax.tree.map(lambda total, term: total + term.astype(jnp.float32), so_far, back(by_y)[0]), None

    none_yet = {name: jnp.zeros(w.shape, jnp.float32) for name, w in weights.items()}
    by_weights, _ = lax.scan(take, none_yet, (x, dy))
    gradients = [by_weights[name].astype(jnp.bfloat16).astype(jnp.float32) for name in NAMES]
    gradients = clipped(gradients, sum(jnp.sum(g * g) for g in gradients), sum(g.size for g in gradients))
    new = [
        adamw(w.astype(jnp.float32), m, v, g)
        for w, m, v, g in zip((w_gate, w_up, w_down), (m_w_gate, m_w_up, m_w_down), (v_w_gate, v_w_up, v_w_down), gradients, strict=True)
    ]
    return tuple(one[which] for which in range(3) for one in new)
```

```python
import functools

import jax
import jax.numpy as jnp
from jax import lax
from jax.experimental import pallas as pl
from jax.experimental.pallas import tpu as pltpu
from jax.sharding import PartitionSpec as P

NAMES = ("w_gate", "w_up", "w_down")
D, FF, LAYERS = 640, 2048, 2
BLOCK = 256
BLOCKS = FF // BLOCK
SUBS = 2
ROWS = D // 2 // SUBS
K = LAYERS * BLOCKS * SUBS
LAG = 2
MESH = pl.DeviceIdType.MESH


def matmul(a, w):
    return jnp.dot(a, w, preferred_element_type=jnp.float32).astype(jnp.bfloat16)


def normed(h):
    wide = h.astype(jnp.float32)
    scale = lax.rsqrt(jnp.mean(wide**2, -1, keepdims=True) + 1e-6)
    return (wide * scale).astype(jnp.bfloat16)


def layer(h, w):
    a = normed(h)
    gate = jnp.dot(a, w["w_gate"], preferred_element_type=jnp.float32)
    up = jnp.dot(a, w["w_up"], preferred_element_type=jnp.float32)
    return h + matmul((jax.nn.silu(gate) * up).astype(jnp.bfloat16), w["w_down"])


def spot(ref, half, q):
    block = q // SUBS
    rows = pl.ds(pl.multiple_of(half * (D // 2) + (q % SUBS) * ROWS, ROWS), ROWS)
    columns = pl.ds(pl.multiple_of((block % BLOCKS) * BLOCK, BLOCK), BLOCK)
    return ref.at[LAYERS - 1 - block // BLOCKS, :, rows, columns]


def reduce_kernel(terms, total, squares, mine, theirs, running, sq, load, pair_s, pair_r, chain_s, chain_r, back_s, back_r, over_s, over_r, out_s, sq_s, sq_r):
    rep, dp = lax.axis_index("rep"), lax.axis_index("dp")
    z, c = dp // 2, dp % 2
    place = z + c * (3 - 2 * z)
    partner = (rep, z * 2 + 1 - c)
    after = (rep, (z + 1 - 2 * c) * 2 + c)
    before = (rep, (z - 1 + 2 * c) * 2 + c)
    barrier = pltpu.get_barrier_semaphore()

    def greet(device):
        pl.semaphore_signal(barrier, inc=1, device_id=device, device_id_type=MESH)

    def remote(source, target, s, r, device):
        return pltpu.make_async_remote_copy(src_ref=source, dst_ref=target, send_sem=s, recv_sem=r, device_id=device, device_id_type=MESH)

    greet(partner)
    pl.when(place < 3)(lambda: greet(after))
    pl.when(place > 0)(lambda: greet(before))
    inner = (place > 0) & (place < 3)
    pl.when(inner)(lambda: pl.semaphore_wait(barrier, 3))
    pl.when(jnp.logical_not(inner))(lambda: pl.semaphore_wait(barrier, 2))

    def loads(q):
        return [pltpu.make_async_copy(spot(terms, half, q), mine.at[half, q], load.at[half, q]) for half in range(2)]

    def pair(q):
        return remote(mine.at[1 - c, q], theirs.at[q], pair_s, pair_r.at[q], partner)

    def chain(q):
        return remote(running.at[q], running.at[q], chain_s, chain_r.at[q], after)

    def back(q):
        return remote(mine.at[c, q], mine.at[c, q], back_s, back_r.at[q], before)

    def over(q):
        return remote(mine.at[c, q], spot(total, c, q), over_s, over_r, partner)

    def out(q):
        return pltpu.make_async_copy(mine.at[c, q], spot(total, c, q), out_s)

    sq[...] = jnp.zeros_like(sq)

    def finished(q):
        pl.when(place > 0)(lambda: back(q).start())
        over(q).start()
        out(q).start()
        g = mine[c, q].astype(jnp.float32).reshape(3 * ROWS // 8, 8, BLOCK)
        s = jnp.sum(g * g, axis=0)
        sq[c] += s[:, :128] + s[:, 128:]

    def add(q):
        pair(q).wait_recv()
        own = mine[c, q].astype(jnp.float32) + theirs[q].astype(jnp.float32)

        @pl.when(place == 0)
        def _():
            running[q] = own.astype(jnp.bfloat16)

        @pl.when(place > 0)
        def _():
            chain(q).wait_recv()

        @pl.when(inner)
        def _():
            running[q] = (own + running[q].astype(jnp.float32)).astype(jnp.bfloat16)

        @pl.when(place == 3)
        def _():
            mine[c, q] = (own + running[q].astype(jnp.float32)).astype(jnp.bfloat16)
            finished(q)

        pl.when(place < 3)(lambda: chain(q).start())

    def service(i):
        q = i - LAG * place
        pl.when((q >= 0) & (q < K))(lambda: add(q))
        r = i - 3 * LAG - LAG * (3 - place)

        @pl.when((r >= 0) & (r < K) & (place < 3))
        def _():
            back(r).wait_recv()
            finished(r)

    def fetch(q, _):
        for copy in loads(q):
            copy.start()
        return 0

    lax.fori_loop(0, K, fetch, 0)

    def ready(i, _):
        for copy in loads(i):
            copy.wait()
        pair(i).start()
        pl.when(i > 0)(lambda: service(i - 1))
        return 0

    lax.fori_loop(0, K, ready, 0)

    def drain(i, _):
        service(i)
        return 0

    lax.fori_loop(K - 1, K + 6 * LAG, drain, 0)

    exchange = remote(sq.at[c], sq.at[c], sq_s, sq_r, partner)
    exchange.start()
    pltpu.make_async_copy(theirs, theirs, pair_s).wait()
    pl.when(place < 3)(lambda: pltpu.make_async_copy(running, running, chain_s).wait())
    pl.when(place > 0)(lambda: pltpu.make_async_copy(running, running, back_s).wait())
    pltpu.make_async_copy(running, running, over_s).wait()
    pltpu.make_async_copy(running, running, over_r).wait()
    pltpu.make_async_copy(running, running, out_s).wait()
    exchange.wait_send()
    remote(sq.at[1 - c], sq.at[1 - c], sq_s, sq_r, partner).wait_recv()
    squares[...] = sq[...]


def summed(terms):
    piece = (3, ROWS, BLOCK)
    dma = pltpu.SemaphoreType.DMA
    return pl.pallas_call(
        reduce_kernel,
        out_shape=(jax.ShapeDtypeStruct(terms.shape, jnp.bfloat16), jax.ShapeDtypeStruct((2, 8, 128), jnp.float32)),
        in_specs=[pl.BlockSpec(memory_space=pl.ANY)],
        out_specs=(pl.BlockSpec(memory_space=pl.ANY), pl.BlockSpec(memory_space=pltpu.VMEM)),
        scratch_shapes=[
            pltpu.VMEM((2, K, *piece), jnp.bfloat16),
            pltpu.VMEM((K, *piece), jnp.bfloat16),
            pltpu.VMEM((K, *piece), jnp.bfloat16),
            pltpu.VMEM((2, 8, 128), jnp.float32),
            dma((2, K)),
            dma, dma((K,)), dma, dma((K,)), dma, dma((K,)), dma, dma, dma, dma, dma,
        ],
        compiler_params=pltpu.CompilerParams(collective_id=0, has_side_effects=True, vmem_limit_bytes=60 * 2**20),
        name="summed",
    )(terms)


def adamw(w, m, v, g):
    m = 0.9 * m + 0.1 * g
    v = 0.95 * v + 0.05 * g * g
    step = m * lax.rsqrt(v + 1e-8) + 0.1 * w
    return (w - 0.02 * step).astype(jnp.bfloat16), m, v


def step_kernel(squares, g, *refs):
    ins, outs = refs[:9], refs[9:]
    factor = jnp.minimum(1.0, 0.5 * lax.rsqrt(jnp.sum(squares[...]) / (3 * LAYERS * D * FF) + 1e-30))
    for i in range(3):
        gradient = g[0, i].astype(jnp.float32)
        if i == 2:
            gradient = gradient.T
        new = adamw(ins[i][0].astype(jnp.float32), ins[3 + i][0], ins[6 + i][0], gradient * factor)
        for which in range(3):
            outs[3 * which + i][0] = new[which]


def stepped(squares, g, arrays):
    wide = pl.BlockSpec((1, D, BLOCK), lambda l, b: (l, 0, b))
    tall = pl.BlockSpec((1, BLOCK, D), lambda l, b: (l, b, 0))
    three = [wide, wide, tall] * 3
    return pl.pallas_call(
        step_kernel,
        grid=(LAYERS, BLOCKS),
        out_shape=[jax.ShapeDtypeStruct(a.shape, a.dtype) for a in arrays],
        in_specs=[
            pl.BlockSpec((2, 8, 128), lambda l, b: (0, 0, 0)),
            pl.BlockSpec((1, 3, D, BLOCK), lambda l, b: (l, 0, 0, b)),
            *three,
        ],
        out_specs=three,
        compiler_params=pltpu.CompilerParams(vmem_limit_bytes=56 * 2**20),
        name="stepped",
    )(squares, g, *arrays)


def solution(mesh):
    def step(x, dy, *arrays):
        weights = arrays[:3]
        h, kept = x[0], []
        for number in range(LAYERS):
            kept.append(h)
            h = layer(h, {name: w[number] for name, w in zip(NAMES, weights, strict=True)})
        by_h, terms = dy[0], [None] * LAYERS
        for number in reversed(range(LAYERS)):
            _, back = jax.vjp(lambda w, h: layer(h, w), {name: w[number] for name, w in zip(NAMES, weights, strict=True)}, kept[number])
            by_w, by_h = back(by_h)
            terms[number] = jnp.stack([by_w["w_gate"], by_w["w_up"], by_w["w_down"].T])
        g, squares = summed(jnp.stack(terms))
        return tuple(stepped(squares, g, arrays))

    return jax.shard_map(
        step,
        mesh=mesh,
        in_specs=(P(("rep", "dp"), None, None),) * 2 + (P(None, None, None),) * 9,
        out_specs=(P("rep", None, None),) * 9,
        check_vma=False,
    )
```

```python
import jax
import jax.numpy as jnp
from jax import lax
from jax.experimental import pallas as pl
from jax.experimental.pallas import tpu as pltpu
from jax.sharding import PartitionSpec as P

TOKENS, D, FF, LAYERS = 2048, 640, 2048, 2
BLOCK = 256
BLOCKS = FF // BLOCK
SUBS = 2
ROWS = D // 2 // SUBS
K = LAYERS * BLOCKS * SUBS
LAG = 2
TILE = 512
MESH = pl.DeviceIdType.MESH


def spot(ref, half, q):
    block = q // SUBS
    rows = pl.ds(pl.multiple_of(half * (D // 2) + (q % SUBS) * ROWS, ROWS), ROWS)
    columns = pl.ds(pl.multiple_of((block % BLOCKS) * BLOCK, BLOCK), BLOCK)
    return ref.at[LAYERS - 1 - block // BLOCKS, :, rows, columns]


def dot(a, b):
    return jnp.dot(a, b, preferred_element_type=jnp.float32)


def dot_t(a, b):
    return lax.dot_general(a, b, (((1,), (1,)), ((), ())), preferred_element_type=jnp.float32)


def half_up(x):
    return x.astype(jnp.bfloat16)


def scale_of(wide):
    return lax.rsqrt(jnp.mean(wide * wide, -1, keepdims=True) + 1e-6)


def train_kernel(
    x_hbm, dy_hbm, gate_hbm, up_hbm, down_hbm, total, squares,
    mine, theirs, running, sq, h, a_first, a_last, a_t, dy, dy_t, acc, product, by_gu, w_gu, w_d,
    w_sem, in_sem, pair_s, pair_r, chain_s, chain_r, back_s, back_r, over_s, over_r, out_s, sq_s, sq_r,
):
    rep, dp = lax.axis_index("rep"), lax.axis_index("dp")
    z, c = dp // 2, dp % 2
    place = z + c * (3 - 2 * z)
    partner = (rep, z * 2 + 1 - c)
    after = (rep, (z + 1 - 2 * c) * 2 + c)
    before = (rep, (z - 1 + 2 * c) * 2 + c)
    inner = (place > 0) & (place < 3)
    barrier = pltpu.get_barrier_semaphore()

    def greet(device):
        pl.semaphore_signal(barrier, inc=1, device_id=device, device_id_type=MESH)

    def remote(source, target, s, r, device):
        return pltpu.make_async_remote_copy(src_ref=source, dst_ref=target, send_sem=s, recv_sem=r, device_id=device, device_id_type=MESH)

    def weights(j):
        number, slot = (j // BLOCKS) % 2, j % 2
        columns = pl.ds(pl.multiple_of((j % BLOCKS) * BLOCK, BLOCK), BLOCK)
        return [
            pltpu.make_async_copy(gate_hbm.at[number, :, columns], w_gu.at[slot, :, pl.ds(0, BLOCK)], w_sem.at[slot, 0]),
            pltpu.make_async_copy(up_hbm.at[number, :, columns], w_gu.at[slot, :, pl.ds(BLOCK, BLOCK)], w_sem.at[slot, 1]),
            pltpu.make_async_copy(down_hbm.at[number, columns, :], w_d.at[slot], w_sem.at[slot, 2]),
        ]

    def next_weights(j):
        for copy in weights(j):
            copy.wait()

        @pl.when(j + 1 < 3 * BLOCKS)
        def _():
            for copy in weights(j + 1):
                copy.start()

    inputs = [pltpu.make_async_copy(x_hbm, h, in_sem.at[0]), pltpu.make_async_copy(dy_hbm, dy, in_sem.at[1])]
    for copy in inputs + weights(0):
        copy.start()
    greet(partner)
    pl.when(place < 3)(lambda: greet(after))
    pl.when(place > 0)(lambda: greet(before))
    pl.when(inner)(lambda: pl.semaphore_wait(barrier, 3))
    pl.when(jnp.logical_not(inner))(lambda: pl.semaphore_wait(barrier, 2))

    def pair(q):
        return remote(mine.at[1 - c, q], theirs.at[q], pair_s, pair_r.at[q], partner)

    def chain(q):
        return remote(running.at[q], running.at[q], chain_s, chain_r.at[q], after)

    def back(q):
        return remote(mine.at[c, q], mine.at[c, q], back_s, back_r.at[q], before)

    def over(q):
        return remote(mine.at[c, q], spot(total, c, q), over_s, over_r, partner)

    def out(q):
        return pltpu.make_async_copy(mine.at[c, q], spot(total, c, q), out_s)

    sq[...] = jnp.zeros_like(sq)

    def finished(q):
        pl.when(place > 0)(lambda: back(q).start())
        over(q).start()
        out(q).start()
        g = mine[c, q].astype(jnp.float32).reshape(3 * ROWS // 8, 8, BLOCK)
        s = jnp.sum(g * g, axis=0)
        sq[c] += s[:, :128] + s[:, 128:]

    def add(q):
        pair(q).wait_recv()
        own = mine[c, q].astype(jnp.float32) + theirs[q].astype(jnp.float32)

        @pl.when(place == 0)
        def _():
            running[q] = half_up(own)

        @pl.when(place > 0)
        def _():
            chain(q).wait_recv()

        @pl.when(inner)
        def _():
            running[q] = half_up(own + running[q].astype(jnp.float32))

        @pl.when(place == 3)
        def _():
            mine[c, q] = half_up(own + running[q].astype(jnp.float32))
            finished(q)

        pl.when(place < 3)(lambda: chain(q).start())

    def service(i):
        q = i - LAG * place
        pl.when((q >= 0) & (q < K))(lambda: add(q))
        r = i - 3 * LAG - LAG * (3 - place)

        @pl.when((r >= 0) & (r < K) & (place < 3))
        def _():
            back(r).wait_recv()
            finished(r)

    def tiles(size, body):
        def at(t, _):
            body(pl.ds(pl.multiple_of(t * size, size), size))
            return 0

        lax.fori_loop(0, TOKENS // size, at, 0)

    for copy in inputs:
        copy.wait()

    def enter(rows):
        wide = h[rows, :].astype(jnp.float32)
        a_first[rows, :] = half_up(wide * scale_of(wide))
        dy_t[:, rows] = half_up(dy[rows, :].astype(jnp.float32).T)
        acc[rows, :] = jnp.zeros_like(acc[rows, :])

    tiles(256, enter)

    def forward(j, _):
        next_weights(j)
        slot = j % 2

        def body(rows):
            both = dot(a_first[rows, :], w_gu[slot])
            gate, up = both[:, :BLOCK], both[:, BLOCK:]
            sigmoid = 0.5 * jnp.tanh(0.5 * gate) + 0.5
            acc[rows, :] += dot(half_up(gate * sigmoid * up), w_d[slot])

        tiles(TILE, body)
        return 0

    lax.fori_loop(0, BLOCKS, forward, 0)

    def between(rows):
        wide = h[rows, :].astype(jnp.float32) + half_up(acc[rows, :]).astype(jnp.float32)
        h[rows, :] = half_up(wide)
        wide = half_up(wide).astype(jnp.float32)
        a = wide * scale_of(wide)
        a_last[rows, :] = half_up(a)
        a_t[:, rows] = half_up(a.T)
        acc[rows, :] = jnp.zeros_like(acc[rows, :])

    tiles(256, between)

    def backward(n, last):
        next_weights(BLOCKS + n)
        slot = n % 2
        a = a_last if last else a_first

        def body(rows):
            both = dot(a[rows, :], w_gu[slot])
            gate, up = both[:, :BLOCK], both[:, BLOCK:]
            by_product = half_up(dot_t(dy[rows, :], w_d[slot])).astype(jnp.float32)
            sigmoid = 0.5 * jnp.tanh(0.5 * gate) + 0.5
            silu = gate * sigmoid
            product[rows, :] = half_up(silu * up)
            by_up = half_up(by_product * silu)
            by_gate = half_up(by_product * up * (sigmoid + silu * (1.0 - sigmoid)))
            by_both = jnp.concatenate([by_gate, by_up], axis=1)
            by_gu[rows, :] = by_both
            if last:
                acc[rows, :] += dot_t(by_both, w_gu[slot])

        per = TOKENS // TILE // SUBS

        def part(s, _):
            for t in range(per):
                body(pl.ds(pl.multiple_of((s * per + t) * TILE, TILE), TILE))
            service(SUBS * n - SUBS + s)
            return 0

        lax.fori_loop(0, SUBS, part, 0)

        def gradient(s, _):
            rows = pl.ds(pl.multiple_of(s * ROWS, ROWS), ROWS)
            place_in = mine.at[s // SUBS, SUBS * n + s % SUBS]
            both = half_up(dot(a_t[rows, :], by_gu[...]))
            place_in[0] = both[:, :BLOCK]
            place_in[1] = both[:, BLOCK:]
            place_in[2] = half_up(dot(dy_t[rows, :], product[...]))
            return 0

        lax.fori_loop(0, 2 * SUBS, gradient, 0)
        for s in range(SUBS):
            pair(SUBS * n + s).start()
        return 0

    lax.fori_loop(0, BLOCKS, lambda n, _: backward(n, True), 0)

    def turn(rows):
        wide = h[rows, :].astype(jnp.float32)
        scale = scale_of(wide)
        by_a = half_up(acc[rows, :]).astype(jnp.float32)
        by_wide = by_a * scale - wide * (scale * scale * scale * jnp.mean(by_a * wide, -1, keepdims=True))
        by_h = dy[rows, :].astype(jnp.float32) + half_up(by_wide).astype(jnp.float32)
        dy[rows, :] = half_up(by_h)
        dy_t[:, rows] = half_up(by_h.T)
        a_t[:, rows] = half_up(a_first[rows, :].astype(jnp.float32).T)

    tiles(256, turn)
    lax.fori_loop(BLOCKS, 2 * BLOCKS, lambda n, _: backward(n, False), 0)

    def drain(i, _):
        service(i)
        return 0

    lax.fori_loop(K - SUBS, K + 6 * LAG, drain, 0)

    exchange = remote(sq.at[c], sq.at[c], sq_s, sq_r, partner)
    exchange.start()
    pltpu.make_async_copy(theirs, theirs, pair_s).wait()
    pl.when(place < 3)(lambda: pltpu.make_async_copy(running, running, chain_s).wait())
    pl.when(place > 0)(lambda: pltpu.make_async_copy(running, running, back_s).wait())
    pltpu.make_async_copy(running, running, over_s).wait()
    pltpu.make_async_copy(running, running, over_r).wait()
    pltpu.make_async_copy(running, running, out_s).wait()
    exchange.wait_send()
    remote(sq.at[1 - c], sq.at[1 - c], sq_s, sq_r, partner).wait_recv()
    squares[...] = sq[...]


def trained(x, dy, gate, up, down):
    piece = (3, ROWS, BLOCK)
    dma = pltpu.SemaphoreType.DMA
    half, full = jnp.bfloat16, jnp.float32
    anywhere = pl.BlockSpec(memory_space=pl.ANY)
    return pl.pallas_call(
        train_kernel,
        out_shape=(jax.ShapeDtypeStruct((LAYERS, 3, D, FF), half), jax.ShapeDtypeStruct((2, 8, 128), full)),
        in_specs=[anywhere] * 5,
        out_specs=(anywhere, pl.BlockSpec(memory_space=pltpu.VMEM)),
        scratch_shapes=[
            pltpu.VMEM((2, K, *piece), half),
            pltpu.VMEM((K, *piece), half),
            pltpu.VMEM((K, *piece), half),
            pltpu.VMEM((2, 8, 128), full),
            pltpu.VMEM((TOKENS, D), half),
            pltpu.VMEM((TOKENS, D), half),
            pltpu.VMEM((TOKENS, D), half),
            pltpu.VMEM((D, TOKENS), half),
            pltpu.VMEM((TOKENS, D), half),
            pltpu.VMEM((D, TOKENS), half),
            pltpu.VMEM((TOKENS, D), full),
            pltpu.VMEM((TOKENS, BLOCK), half),
            pltpu.VMEM((TOKENS, 2 * BLOCK), half),
            pltpu.VMEM((2, D, 2 * BLOCK), half),
            pltpu.VMEM((2, BLOCK, D), half),
            dma((2, 3)), dma((2,)),
            dma, dma((K,)), dma, dma((K,)), dma, dma((K,)), dma, dma, dma, dma, dma,
        ],
        compiler_params=pltpu.CompilerParams(collective_id=0, has_side_effects=True, vmem_limit_bytes=67043328),
        name="trained",
    )(x, dy, gate, up, down)


def adamw(w, m, v, g):
    m = 0.9 * m + 0.1 * g
    v = 0.95 * v + 0.05 * g * g
    step = m * lax.rsqrt(v + 1e-8) + 0.1 * w
    return (w - 0.02 * step).astype(jnp.bfloat16), m, v


def step_kernel(squares, g, *refs):
    ins, outs = refs[:9], refs[9:]
    factor = jnp.minimum(1.0, 0.5 * lax.rsqrt(jnp.sum(squares[...]) / (3 * LAYERS * D * FF) + 1e-30))
    for i in range(3):
        gradient = g[0, i].astype(jnp.float32)
        if i == 2:
            gradient = gradient.T
        new = adamw(ins[i][0].astype(jnp.float32), ins[3 + i][0], ins[6 + i][0], gradient * factor)
        for which in range(3):
            outs[3 * which + i][0] = new[which]


def stepped(squares, g, arrays):
    wide = pl.BlockSpec((1, D, BLOCK), lambda l, b: (l, 0, b))
    tall = pl.BlockSpec((1, BLOCK, D), lambda l, b: (l, b, 0))
    three = [wide, wide, tall] * 3
    return pl.pallas_call(
        step_kernel,
        grid=(LAYERS, BLOCKS),
        out_shape=[jax.ShapeDtypeStruct(a.shape, a.dtype) for a in arrays],
        in_specs=[
            pl.BlockSpec((2, 8, 128), lambda l, b: (0, 0, 0)),
            pl.BlockSpec((1, 3, D, BLOCK), lambda l, b: (l, 0, 0, b)),
            *three,
        ],
        out_specs=three,
        compiler_params=pltpu.CompilerParams(vmem_limit_bytes=56 * 2**20),
        name="stepped",
    )(squares, g, *arrays)


def solution(mesh):
    def step(x, dy, *arrays):
        g, squares = trained(x[0], dy[0], *arrays[:3])
        return tuple(stepped(squares, g, arrays))

    return jax.shard_map(
        step,
        mesh=mesh,
        in_specs=(P(("rep", "dp"), None, None),) * 2 + (P(None, None, None),) * 9,
        out_specs=(P("rep", None, None),) * 9,
        check_vma=False,
    )
```

```python
import jax
import jax.numpy as jnp
from jax import lax
from jax.experimental import pallas as pl
from jax.experimental.pallas import tpu as pltpu
from jax.sharding import PartitionSpec as P

TOKENS, D, FF, LAYERS = 2048, 640, 2048, 2
BLOCK = 256
BLOCKS = FF // BLOCK
STEP = 512
SUBS = 4
PARTS = 4
ROWS = D // 2 // SUBS
K = LAYERS * BLOCKS * SUBS
LAG, BACK_LAG = 3, 2
TILE, FORWARD_TILE = 512, 1024
MESH = pl.DeviceIdType.MESH


def spot(ref, half, q):
    block = q // SUBS
    rows = pl.ds(pl.multiple_of(half * (D // 2) + (q % SUBS) * ROWS, ROWS), ROWS)
    columns = pl.ds(pl.multiple_of((block % BLOCKS) * BLOCK, BLOCK), BLOCK)
    return ref.at[LAYERS - 1 - block // BLOCKS, :, rows, columns]


def dot(a, b):
    return jnp.dot(a, b, preferred_element_type=jnp.float32)


def dot_t(a, b):
    return lax.dot_general(a, b, (((1,), (1,)), ((), ())), preferred_element_type=jnp.float32)


def half_up(x):
    return x.astype(jnp.bfloat16)


def scale_of(wide):
    return lax.rsqrt(jnp.mean(wide * wide, -1, keepdims=True) + 1e-6)


def train_kernel(
    x_hbm, dy_hbm, gate_hbm, up_hbm, down_hbm, total, squares,
    mine, theirs, running, sq, h, a_first, a_last, a_t, dy, dy_t, acc, product, by_gu, w_gu, w_d,
    w_sem, in_sem, pair_s, pair_r, chain_s, chain_r, back_s, back_r, over_s, over_r, out_s, sq_s, sq_r,
):
    rep, dp = lax.axis_index("rep"), lax.axis_index("dp")
    z, c = dp // 2, dp % 2
    place = z + c * (3 - 2 * z)
    partner = (rep, z * 2 + 1 - c)
    after = (rep, (z + 1 - 2 * c) * 2 + c)
    before = (rep, (z - 1 + 2 * c) * 2 + c)
    inner = (place > 0) & (place < 3)
    barrier = pltpu.get_barrier_semaphore()

    def greet(device):
        pl.semaphore_signal(barrier, inc=1, device_id=device, device_id_type=MESH)

    def remote(source, target, s, r, device):
        return pltpu.make_async_remote_copy(src_ref=source, dst_ref=target, send_sem=s, recv_sem=r, device_id=device, device_id_type=MESH)

    def weights(j):
        number, slot = (j // BLOCKS) % 2, j % 2
        columns = pl.ds(pl.multiple_of((j % BLOCKS) * BLOCK, BLOCK), BLOCK)
        return [
            pltpu.make_async_copy(gate_hbm.at[number, :, columns], w_gu.at[slot, :, pl.ds(0, BLOCK)], w_sem.at[slot, 0]),
            pltpu.make_async_copy(up_hbm.at[number, :, columns], w_gu.at[slot, :, pl.ds(BLOCK, BLOCK)], w_sem.at[slot, 1]),
            pltpu.make_async_copy(down_hbm.at[number, columns, :], w_d.at[slot], w_sem.at[slot, 2]),
        ]

    def next_weights(j):
        for copy in weights(j):
            copy.wait()

        @pl.when(j + 1 < 3 * BLOCKS)
        def _():
            for copy in weights(j + 1):
                copy.start()

    inputs = [pltpu.make_async_copy(x_hbm, h, in_sem.at[0]), pltpu.make_async_copy(dy_hbm, dy, in_sem.at[1])]
    for copy in inputs + weights(0):
        copy.start()
    greet(partner)
    pl.when(place < 3)(lambda: greet(after))
    pl.when(place > 0)(lambda: greet(before))
    pl.when(inner)(lambda: pl.semaphore_wait(barrier, 3))
    pl.when(jnp.logical_not(inner))(lambda: pl.semaphore_wait(barrier, 2))

    def pair(q):
        return remote(mine.at[1 - c, q], theirs.at[q], pair_s, pair_r.at[q], partner)

    def chain(q):
        return remote(running.at[q], running.at[q], chain_s, chain_r.at[q], after)

    def back(q):
        return remote(mine.at[c, q], mine.at[c, q], back_s, back_r.at[q], before)

    def over(q):
        return remote(mine.at[c, q], spot(total, c, q), over_s, over_r, partner)

    def out(q):
        return pltpu.make_async_copy(mine.at[c, q], spot(total, c, q), out_s)

    sq[...] = jnp.zeros_like(sq)

    def finished(q):
        pl.when(place > 0)(lambda: back(q).start())
        over(q).start()
        out(q).start()
        g = mine[c, q].astype(jnp.float32).reshape(3 * ROWS // 8, 8, BLOCK)
        s = jnp.sum(g * g, axis=0)
        sq[c] += s[:, :128] + s[:, 128:]

    def add(q):
        pair(q).wait_recv()
        own = mine[c, q].astype(jnp.float32) + theirs[q].astype(jnp.float32)

        @pl.when(place == 0)
        def _():
            running[q] = half_up(own)

        @pl.when(place > 0)
        def _():
            chain(q).wait_recv()

        @pl.when(inner)
        def _():
            running[q] = half_up(own + running[q].astype(jnp.float32))

        @pl.when(place == 3)
        def _():
            mine[c, q] = half_up(own + running[q].astype(jnp.float32))
            finished(q)

        pl.when(place < 3)(lambda: chain(q).start())

    def service(i):
        q = i - LAG * place
        pl.when((q >= 0) & (q < K))(lambda: add(q))
        r = i - 3 * LAG - BACK_LAG * (3 - place)

        @pl.when((r >= 0) & (r < K) & (place < 3))
        def _():
            back(r).wait_recv()
            finished(r)

    def tiles(size, body):
        def at(t, _):
            body(pl.ds(pl.multiple_of(t * size, size), size))
            return 0

        lax.fori_loop(0, TOKENS // size, at, 0)

    for copy in inputs:
        copy.wait()

    def enter(rows):
        wide = h[rows, :].astype(jnp.float32)
        a_first[rows, :] = half_up(wide * scale_of(wide))
        acc[rows, :] = jnp.zeros_like(acc[rows, :])

    tiles(256, enter)

    def forward(j, _):
        next_weights(j)
        slot = j % 2

        def body(rows):
            both = dot(a_first[rows, :], w_gu[slot])
            gate, up = both[:, :BLOCK], both[:, BLOCK:]
            sigmoid = 0.5 * jnp.tanh(0.5 * gate) + 0.5
            acc[rows, :] += dot(half_up(gate * sigmoid * up), w_d[slot])

            turned = pl.ds(pl.multiple_of(j * (TOKENS // BLOCKS) + rows.start // BLOCKS, 128), FORWARD_TILE // BLOCKS)
            dy_t[:, turned] = half_up(dy[turned, :].astype(jnp.float32).T)

        tiles(FORWARD_TILE, body)
        return 0

    lax.fori_loop(0, BLOCKS, forward, 0)

    def between(rows):
        wide = h[rows, :].astype(jnp.float32) + half_up(acc[rows, :]).astype(jnp.float32)
        h[rows, :] = half_up(wide)
        wide = half_up(wide).astype(jnp.float32)
        a = wide * scale_of(wide)
        a_last[rows, :] = half_up(a)
        a_t[:, rows] = half_up(a.T)
        acc[rows, :] = jnp.zeros_like(acc[rows, :])

    tiles(256, between)

    def backward(n, last):
        next_weights(BLOCKS + n)
        slot = n % 2
        a = a_last if last else a_first

        def body(rows):
            both = dot(a[rows, :], w_gu[slot])
            gate, up = both[:, :BLOCK], both[:, BLOCK:]
            by_product = half_up(dot_t(dy[rows, :], w_d[slot])).astype(jnp.float32)
            sigmoid = 0.5 * jnp.tanh(0.5 * gate) + 0.5
            silu = gate * sigmoid
            product[rows, :] = half_up(silu * up)
            by_up = half_up(by_product * silu)
            by_gate = half_up(by_product * up * (sigmoid + silu * (1.0 - sigmoid)))
            by_both = jnp.concatenate([by_gate, by_up], axis=1)
            by_gu[rows, :] = by_both
            if last:
                acc[rows, :] += dot_t(by_both, w_gu[slot])

        per = TOKENS // TILE // PARTS

        def part(s, _):
            for t in range(per):
                body(pl.ds(pl.multiple_of((s * per + t) * TILE, TILE), TILE))
            for t in range(SUBS // PARTS):
                service(SUBS * (n - 1) + s * (SUBS // PARTS) + t)
            return 0

        lax.fori_loop(0, PARTS, part, 0)

        def gradient(half, _):
            rows = pl.ds(pl.multiple_of(half * (D // 2), D // 2), D // 2)
            both = half_up(dot(a_t[rows, :], by_gu[...]))
            down = half_up(dot(dy_t[rows, :], product[...]))
            for s in range(SUBS):
                here = slice(s * ROWS, (s + 1) * ROWS)
                mine[half, SUBS * n + s, 0] = both[here, :BLOCK]
                mine[half, SUBS * n + s, 1] = both[here, BLOCK:]
                mine[half, SUBS * n + s, 2] = down[here]
            return 0

        lax.fori_loop(0, 2, gradient, 0)
        for s in range(SUBS):
            pair(SUBS * n + s).start()
        return 0

    lax.fori_loop(0, BLOCKS, lambda n, _: backward(n, True), 0)

    def turn(rows):
        wide = h[rows, :].astype(jnp.float32)
        scale = scale_of(wide)
        by_a = half_up(acc[rows, :]).astype(jnp.float32)
        by_wide = by_a * scale - wide * (scale * scale * scale * jnp.mean(by_a * wide, -1, keepdims=True))
        by_h = dy[rows, :].astype(jnp.float32) + half_up(by_wide).astype(jnp.float32)
        dy[rows, :] = half_up(by_h)
        dy_t[:, rows] = half_up(by_h.T)
        a_t[:, rows] = half_up(a_first[rows, :].astype(jnp.float32).T)

    tiles(256, turn)
    lax.fori_loop(BLOCKS, 2 * BLOCKS, lambda n, _: backward(n, False), 0)

    def drain(i, _):
        service(i)
        return 0

    lax.fori_loop(K - SUBS, K + 3 * (LAG + BACK_LAG), drain, 0)

    exchange = remote(sq.at[c], sq.at[c], sq_s, sq_r, partner)
    exchange.start()
    pltpu.make_async_copy(theirs, theirs, pair_s).wait()
    pl.when(place < 3)(lambda: pltpu.make_async_copy(running, running, chain_s).wait())
    pl.when(place > 0)(lambda: pltpu.make_async_copy(running, running, back_s).wait())
    pltpu.make_async_copy(running, running, over_s).wait()
    pltpu.make_async_copy(running, running, over_r).wait()
    pltpu.make_async_copy(running, running, out_s).wait()
    exchange.wait_send()
    remote(sq.at[1 - c], sq.at[1 - c], sq_s, sq_r, partner).wait_recv()
    squares[...] = sq[...]


def trained(x, dy, gate, up, down):
    piece = (3, ROWS, BLOCK)
    dma = pltpu.SemaphoreType.DMA
    half, full = jnp.bfloat16, jnp.float32
    anywhere = pl.BlockSpec(memory_space=pl.ANY)
    return pl.pallas_call(
        train_kernel,
        out_shape=(jax.ShapeDtypeStruct((LAYERS, 3, D, FF), half), jax.ShapeDtypeStruct((2, 8, 128), full)),
        in_specs=[anywhere] * 5,
        out_specs=(anywhere, pl.BlockSpec(memory_space=pltpu.VMEM)),
        scratch_shapes=[
            pltpu.VMEM((2, K, *piece), half),
            pltpu.VMEM((K, *piece), half),
            pltpu.VMEM((K, *piece), half),
            pltpu.VMEM((2, 8, 128), full),
            pltpu.VMEM((TOKENS, D), half),
            pltpu.VMEM((TOKENS, D), half),
            pltpu.VMEM((TOKENS, D), half),
            pltpu.VMEM((D, TOKENS), half),
            pltpu.VMEM((TOKENS, D), half),
            pltpu.VMEM((D, TOKENS), half),
            pltpu.VMEM((TOKENS, D), full),
            pltpu.VMEM((TOKENS, BLOCK), half),
            pltpu.VMEM((TOKENS, 2 * BLOCK), half),
            pltpu.VMEM((2, D, 2 * BLOCK), half),
            pltpu.VMEM((2, BLOCK, D), half),
            dma((2, 3)), dma((2,)),
            dma, dma((K,)), dma, dma((K,)), dma, dma((K,)), dma, dma, dma, dma, dma,
        ],
        compiler_params=pltpu.CompilerParams(collective_id=0, has_side_effects=True, vmem_limit_bytes=67043328),
        name="trained",
    )(x, dy, gate, up, down)


def adamw(w, m, v, g):
    m = 0.9 * m + 0.1 * g
    v = 0.95 * v + 0.05 * g * g
    step = m * lax.rsqrt(v + 1e-8) + 0.1 * w
    return (w - 0.02 * step).astype(jnp.bfloat16), m, v


def step_kernel(squares, g, *refs):
    ins, outs = refs[:9], refs[9:]
    factor = jnp.minimum(1.0, 0.5 * lax.rsqrt(jnp.sum(squares[...]) / (3 * LAYERS * D * FF) + 1e-30))
    for i in range(3):
        gradient = g[0, i].astype(jnp.float32)
        if i == 2:
            gradient = gradient.T
        new = adamw(ins[i][0].astype(jnp.float32), ins[3 + i][0], ins[6 + i][0], gradient * factor)
        for which in range(3):
            outs[3 * which + i][0] = new[which]


def stepped(squares, g, arrays):
    wide = pl.BlockSpec((1, D, STEP), lambda l, b: (l, 0, b))
    tall = pl.BlockSpec((1, STEP, D), lambda l, b: (l, b, 0))
    three = [wide, wide, tall] * 3
    return pl.pallas_call(
        step_kernel,
        grid=(LAYERS, FF // STEP),
        out_shape=[jax.ShapeDtypeStruct(a.shape, a.dtype) for a in arrays],
        in_specs=[
            pl.BlockSpec((2, 8, 128), lambda l, b: (0, 0, 0)),
            pl.BlockSpec((1, 3, D, STEP), lambda l, b: (l, 0, 0, b)),
            *three,
        ],
        out_specs=three,
        compiler_params=pltpu.CompilerParams(vmem_limit_bytes=56 * 2**20),
        name="stepped",
    )(squares, g, *arrays)


def solution(mesh):
    def step(x, dy, *arrays):
        g, squares = trained(x[0], dy[0], *arrays[:3])
        return tuple(stepped(squares, g, arrays))

    return jax.shard_map(
        step,
        mesh=mesh,
        in_specs=(P(("rep", "dp"), None, None),) * 2 + (P(None, None, None),) * 9,
        out_specs=(P("rep", None, None),) * 9,
        check_vma=False,
    )
```

```python
import jax
import jax.numpy as jnp
from jax import lax
from jax.experimental import pallas as pl
from jax.experimental.pallas import tpu as pltpu
from jax.sharding import PartitionSpec as P

TOKENS, D, FF, LAYERS = 2048, 640, 2048, 2
BLOCK = 256
BLOCKS = FF // BLOCK
STEPS = 4
SUBS = 4
PARTS = 4
ROWS = D // 2 // SUBS
K = LAYERS * BLOCKS * SUBS
LAG, BACK_LAG = 3, 2
TILE, FORWARD_TILE = 512, 1024
MESH = pl.DeviceIdType.MESH


def spot(ref, half, q):
    block = q // SUBS
    rows = pl.ds(pl.multiple_of(half * (D // 2) + (q % SUBS) * ROWS, ROWS), ROWS)
    columns = pl.ds(pl.multiple_of((block % BLOCKS) * BLOCK, BLOCK), BLOCK)
    return ref.at[LAYERS - 1 - block // BLOCKS, :, rows, columns]


def dot(a, b):
    return jnp.dot(a, b, preferred_element_type=jnp.float32)


def dot_t(a, b):
    return lax.dot_general(a, b, (((1,), (1,)), ((), ())), preferred_element_type=jnp.float32)


def half_up(x):
    return x.astype(jnp.bfloat16)


def scale_of(wide):
    return lax.rsqrt(jnp.mean(wide * wide, -1, keepdims=True) + 1e-6)


def train_kernel(
    x_hbm, dy_hbm, gate_hbm, up_hbm, down_hbm, total, squares,
    mine, theirs, running, sq, h, a_first, a_last, a_t, dy, dy_t, acc, product, by_gu, w_gu, w_d,
    w_sem, in_sem, pair_s, pair_r, chain_s, chain_r, back_s, back_r, over_s, over_r, out_s, sq_s, sq_r,
):
    rep, dp = lax.axis_index("rep"), lax.axis_index("dp")
    z, c = dp // 2, dp % 2
    place = z + c * (3 - 2 * z)
    partner = (rep, z * 2 + 1 - c)
    after = (rep, (z + 1 - 2 * c) * 2 + c)
    before = (rep, (z - 1 + 2 * c) * 2 + c)
    inner = (place > 0) & (place < 3)
    barrier = pltpu.get_barrier_semaphore()

    def greet(device):
        pl.semaphore_signal(barrier, inc=1, device_id=device, device_id_type=MESH)

    def remote(source, target, s, r, device):
        return pltpu.make_async_remote_copy(src_ref=source, dst_ref=target, send_sem=s, recv_sem=r, device_id=device, device_id_type=MESH)

    def weights(j):
        number, slot = (j // BLOCKS) % 2, j % 2
        columns = pl.ds(pl.multiple_of((j % BLOCKS) * BLOCK, BLOCK), BLOCK)
        return [
            pltpu.make_async_copy(gate_hbm.at[number, :, columns], w_gu.at[slot, :, pl.ds(0, BLOCK)], w_sem.at[slot, 0]),
            pltpu.make_async_copy(up_hbm.at[number, :, columns], w_gu.at[slot, :, pl.ds(BLOCK, BLOCK)], w_sem.at[slot, 1]),
            pltpu.make_async_copy(down_hbm.at[number, columns, :], w_d.at[slot], w_sem.at[slot, 2]),
        ]

    def next_weights(j):
        for copy in weights(j):
            copy.wait()

        @pl.when(j + 1 < 3 * BLOCKS)
        def _():
            for copy in weights(j + 1):
                copy.start()

    inputs = [pltpu.make_async_copy(x_hbm, h, in_sem.at[0]), pltpu.make_async_copy(dy_hbm, dy, in_sem.at[1])]
    for copy in inputs + weights(0):
        copy.start()
    greet(partner)
    pl.when(place < 3)(lambda: greet(after))
    pl.when(place > 0)(lambda: greet(before))
    pl.when(inner)(lambda: pl.semaphore_wait(barrier, 3))
    pl.when(jnp.logical_not(inner))(lambda: pl.semaphore_wait(barrier, 2))

    def pair(q):
        return remote(mine.at[1 - c, q], theirs.at[q], pair_s, pair_r.at[q], partner)

    def chain(q):
        return remote(running.at[q], running.at[q], chain_s, chain_r.at[q], after)

    def back(q):
        return remote(mine.at[c, q], mine.at[c, q], back_s, back_r.at[q], before)

    def over(q):
        return remote(mine.at[c, q], spot(total, c, q), over_s, over_r, partner)

    def out(q):
        return pltpu.make_async_copy(mine.at[c, q], spot(total, c, q), out_s)

    sq[...] = jnp.zeros_like(sq)

    def finished(q):
        pl.when(place > 0)(lambda: back(q).start())
        over(q).start()
        out(q).start()
        g = mine[c, q].astype(jnp.float32).reshape(3 * ROWS // 8, 8, BLOCK)
        s = jnp.sum(g * g, axis=0)
        sq[c] += s[:, :128] + s[:, 128:]

    def add(q):
        pair(q).wait_recv()
        own = mine[c, q].astype(jnp.float32) + theirs[q].astype(jnp.float32)

        @pl.when(place == 0)
        def _():
            running[q] = half_up(own)

        @pl.when(place > 0)
        def _():
            chain(q).wait_recv()

        @pl.when(inner)
        def _():
            running[q] = half_up(own + running[q].astype(jnp.float32))

        @pl.when(place == 3)
        def _():
            mine[c, q] = half_up(own + running[q].astype(jnp.float32))
            finished(q)

        pl.when(place < 3)(lambda: chain(q).start())

    def service(i):
        r = i - 3 * LAG - BACK_LAG * (3 - place)

        @pl.when((r >= 0) & (r < K) & (place < 3))
        def _():
            back(r).wait_recv()
            finished(r)

        q = i - LAG * place
        pl.when((q >= 0) & (q < K))(lambda: add(q))

    def tiles(size, body):
        def at(t, _):
            body(pl.ds(pl.multiple_of(t * size, size), size))
            return 0

        lax.fori_loop(0, TOKENS // size, at, 0)

    def enter(rows):
        wide = h[rows, :].astype(jnp.float32)
        a_first[rows, :] = half_up(wide * scale_of(wide))
        acc[rows, :] = jnp.zeros_like(acc[rows, :])

    inputs[0].wait()
    tiles(512, enter)
    inputs[1].wait()

    def forward(j, _):
        next_weights(j)
        slot = j % 2

        def body(rows):
            both = dot(a_first[rows, :], w_gu[slot])
            gate, up = both[:, :BLOCK], both[:, BLOCK:]
            sigmoid = 0.5 * jnp.tanh(0.5 * gate) + 0.5
            acc[rows, :] += dot(half_up(gate * sigmoid * up), w_d[slot])

            turned = pl.ds(pl.multiple_of(j * (TOKENS // BLOCKS) + rows.start // BLOCKS, 128), FORWARD_TILE // BLOCKS)
            dy_t[:, turned] = half_up(dy[turned, :].astype(jnp.float32).T)

        tiles(FORWARD_TILE, body)
        return 0

    lax.fori_loop(0, BLOCKS, forward, 0)

    def between(rows):
        wide = h[rows, :].astype(jnp.float32) + half_up(acc[rows, :]).astype(jnp.float32)
        h[rows, :] = half_up(wide)
        wide = half_up(wide).astype(jnp.float32)
        a = wide * scale_of(wide)
        a_last[rows, :] = half_up(a)
        a_t[:, rows] = half_up(a.T)
        acc[rows, :] = jnp.zeros_like(acc[rows, :])

    tiles(512, between)

    def backward(n, last):
        next_weights(BLOCKS + n)
        slot = n % 2
        a = a_last if last else a_first

        def body(rows):
            both = dot(a[rows, :], w_gu[slot])
            gate, up = both[:, :BLOCK], both[:, BLOCK:]
            by_product = half_up(dot_t(dy[rows, :], w_d[slot])).astype(jnp.float32)
            sigmoid = 0.5 * jnp.tanh(0.5 * gate) + 0.5
            silu = gate * sigmoid
            product[rows, :] = half_up(silu * up)
            by_up = half_up(by_product * silu)
            by_gate = half_up(by_product * up * (sigmoid + silu * (1.0 - sigmoid)))
            by_both = jnp.concatenate([by_gate, by_up], axis=1)
            by_gu[rows, :] = by_both
            if last:
                acc[rows, :] += dot_t(by_both, w_gu[slot])

        per = TOKENS // TILE // PARTS

        def part(s, _):
            for t in range(per):
                body(pl.ds(pl.multiple_of((s * per + t) * TILE, TILE), TILE))
            for t in range(SUBS // PARTS):
                service(SUBS * (n - 1) + s * (SUBS // PARTS) + t)
            return 0

        lax.fori_loop(0, PARTS, part, 0)

        def gradient(half, _):
            rows = pl.ds(pl.multiple_of(half * (D // 2), D // 2), D // 2)
            both = half_up(dot(a_t[rows, :], by_gu[...]))
            down = half_up(dot(dy_t[rows, :], product[...]))
            for s in range(SUBS):
                here = slice(s * ROWS, (s + 1) * ROWS)
                mine[half, SUBS * n + s, 0] = both[here, :BLOCK]
                mine[half, SUBS * n + s, 1] = both[here, BLOCK:]
                mine[half, SUBS * n + s, 2] = down[here]
            return 0

        lax.fori_loop(0, 2, gradient, 0)
        for s in range(SUBS):
            pair(SUBS * n + s).start()
        return 0

    lax.fori_loop(0, BLOCKS, lambda n, _: backward(n, True), 0)

    def turn(rows):
        wide = h[rows, :].astype(jnp.float32)
        scale = scale_of(wide)
        by_a = half_up(acc[rows, :]).astype(jnp.float32)
        by_wide = by_a * scale - wide * (scale * scale * scale * jnp.mean(by_a * wide, -1, keepdims=True))
        by_h = dy[rows, :].astype(jnp.float32) + half_up(by_wide).astype(jnp.float32)
        dy[rows, :] = half_up(by_h)
        dy_t[:, rows] = half_up(by_h.T)
        a_t[:, rows] = half_up(a_first[rows, :].astype(jnp.float32).T)

    tiles(512, turn)
    lax.fori_loop(BLOCKS, 2 * BLOCKS, lambda n, _: backward(n, False), 0)

    def drain(i, _):
        service(i)
        return 0

    lax.fori_loop(K - SUBS, K + 3 * (LAG + BACK_LAG), drain, 0)

    exchange = remote(sq.at[c], sq.at[c], sq_s, sq_r, partner)
    exchange.start()
    pltpu.make_async_copy(theirs, theirs, pair_s).wait()
    pl.when(place < 3)(lambda: pltpu.make_async_copy(running, running, chain_s).wait())
    pl.when(place > 0)(lambda: pltpu.make_async_copy(running, running, back_s).wait())
    pltpu.make_async_copy(running, running, over_s).wait()
    pltpu.make_async_copy(running, running, over_r).wait()
    pltpu.make_async_copy(running, running, out_s).wait()
    exchange.wait_send()
    remote(sq.at[1 - c], sq.at[1 - c], sq_s, sq_r, partner).wait_recv()
    squares[...] = sq[...]


def trained(x, dy, gate, up, down):
    piece = (3, ROWS, BLOCK)
    dma = pltpu.SemaphoreType.DMA
    half, full = jnp.bfloat16, jnp.float32
    anywhere = pl.BlockSpec(memory_space=pl.ANY)
    return pl.pallas_call(
        train_kernel,
        out_shape=(jax.ShapeDtypeStruct((LAYERS, 3, D, FF), half), jax.ShapeDtypeStruct((2, 8, 128), full)),
        in_specs=[anywhere] * 5,
        out_specs=(anywhere, pl.BlockSpec(memory_space=pltpu.VMEM)),
        scratch_shapes=[
            pltpu.VMEM((2, K, *piece), half),
            pltpu.VMEM((K, *piece), half),
            pltpu.VMEM((K, *piece), half),
            pltpu.VMEM((2, 8, 128), full),
            pltpu.VMEM((TOKENS, D), half),
            pltpu.VMEM((TOKENS, D), half),
            pltpu.VMEM((TOKENS, D), half),
            pltpu.VMEM((D, TOKENS), half),
            pltpu.VMEM((TOKENS, D), half),
            pltpu.VMEM((D, TOKENS), half),
            pltpu.VMEM((TOKENS, D), full),
            pltpu.VMEM((TOKENS, BLOCK), half),
            pltpu.VMEM((TOKENS, 2 * BLOCK), half),
            pltpu.VMEM((2, D, 2 * BLOCK), half),
            pltpu.VMEM((2, BLOCK, D), half),
            dma((2, 3)), dma((2,)),
            dma, dma((K,)), dma, dma((K,)), dma, dma((K,)), dma, dma, dma, dma, dma,
        ],
        compiler_params=pltpu.CompilerParams(collective_id=0, has_side_effects=True, vmem_limit_bytes=67043328),
        name="trained",
    )(x, dy, gate, up, down)


def adamw(w, m, v, g):
    m = 0.9 * m + 0.1 * g
    v = 0.95 * v + 0.05 * g * g
    step = m * lax.rsqrt(v + 1e-8) + 0.1 * w
    return (w - 0.02 * step).astype(jnp.bfloat16), m, v


def step_kernel(squares, g_wide, g_tall, *refs):
    ins, outs = refs[:9], refs[9:]
    factor = jnp.minimum(1.0, 0.5 * lax.rsqrt(jnp.sum(squares[...]) / (3 * LAYERS * D * FF) + 1e-30))
    for i in range(3):
        gradient = g_wide[0, i].astype(jnp.float32) if i < 2 else g_tall[0, 0].astype(jnp.float32).T
        new = adamw(ins[i][0].astype(jnp.float32), ins[3 + i][0], ins[6 + i][0], gradient * factor)
        for which in range(3):
            outs[3 * which + i][0] = new[which]


def stepped(squares, g, arrays):
    wide = pl.BlockSpec((1, D // STEPS, FF), lambda l, b: (l, b, 0))
    tall = pl.BlockSpec((1, FF // STEPS, D), lambda l, b: (l, b, 0))
    three = [wide, wide, tall] * 3
    return pl.pallas_call(
        step_kernel,
        grid=(LAYERS, STEPS),
        out_shape=[jax.ShapeDtypeStruct(a.shape, a.dtype) for a in arrays],
        in_specs=[
            pl.BlockSpec((2, 8, 128), lambda l, b: (0, 0, 0)),
            pl.BlockSpec((1, 2, D // STEPS, FF), lambda l, b: (l, 0, b, 0)),
            pl.BlockSpec((1, 1, D, FF // STEPS), lambda l, b: (l, 2, 0, b)),
            *three,
        ],
        out_specs=three,
        compiler_params=pltpu.CompilerParams(vmem_limit_bytes=56 * 2**20),
        name="stepped",
    )(squares, g, g, *arrays)


def solution(mesh):
    def step(x, dy, *arrays):
        g, squares = trained(x[0], dy[0], *arrays[:3])
        return tuple(stepped(squares, g, arrays))

    return jax.shard_map(
        step,
        mesh=mesh,
        in_specs=(P(("rep", "dp"), None, None),) * 2 + (P(None, None, None),) * 9,
        out_specs=(P("rep", None, None),) * 9,
        check_vma=False,
    )
```
